64 devices in a mesh: dp: 4 (over x, y), ep: 16 (over z, core).
Axes of the slice: x: 2, y: 2, z: 8, core: 2. Of those that a mesh axis runs over, the one named last changes fastest.
The devices are a block of a 4x4x8 slice.
Arguments:
- tokens_a: bfloat16 [4096, 1024], P(('dp', 'ep')), parts along dimension 0
- experts_a: int32 [4096, 8], P(('dp', 'ep')), parts along dimension 0
- slots_a: int32 [4096, 8], P(('dp', 'ep')), parts along dimension 0
- gates_a: bfloat16 [4096, 8], P(('dp', 'ep')), parts along dimension 0
- tokens_b: bfloat16 [4096, 1024], P(('dp', 'ep')), parts along dimension 0
- experts_b: int32 [4096, 8], P(('dp', 'ep')), parts along dimension 0
- slots_b: int32 [4096, 8], P(('dp', 'ep')), parts along dimension 0
- gates_b: bfloat16 [4096, 8], P(('dp', 'ep')), parts along dimension 0
- attn_gain: bfloat16 [1024], replicated
- w_query: bfloat16 [1024, 16, 64], replicated
- w_key: bfloat16 [1024, 16, 64], replicated
- w_value: bfloat16 [1024, 16, 64], replicated
- w_out: bfloat16 [16, 64, 1024], replicated
- moe_gain: bfloat16 [1024], replicated
- w_gate: bfloat16 [32, 1024, 512], P('ep')
- w_up: bfloat16 [32, 1024, 512], P('ep')
- w_down: bfloat16 [32, 512, 1024], P('ep')
Outputs:
- output 1: bfloat16 [4096, 1024], P(('dp', 'ep')), parts along dimension 0
- output 2: bfloat16 [4096, 1024], P(('dp', 'ep')), parts along dimension 0
There are 4 independent parts. The reference program is written for one: setup_inputs(seed, part) draws one part's arguments, and reference() takes and returns one part's arrays. A program takes and returns all parts, laid end to end along the dimension named above; an argument that names none is the same for every part.
All inputs are finite; a program needn't handle non-finite values.
Results may differ from the reference program's by a relative error of at most 0.014492.
Values are sent between devices in bfloat16 or wider.
A program may use at most 768 MiB of HBM per device.

```python
import jax
import jax.numpy as jnp
from jax import lax

MODEL_DIM = 1024
FFN_DIM = 512
EXPERTS = 32
TOP_K = 8
HEADS = 16
TOKENS = 64
GROUP = 16
SLOTS = 32

HEAD_DIM = MODEL_DIM // HEADS
ROWS = GROUP * TOKENS
NORM_EPS = 1e-6
MASK_VALUE = -1e30


def draw_routing(route_key):
    key_start, key_hot, key_pick = jax.random.split(route_key, 3)
    spacing = EXPERTS // TOP_K
    hot_span = max(1, EXPERTS // (4 * TOP_K))
    start_any = jax.random.randint(key_start, (ROWS,), 0, EXPERTS)
    start_hot = jax.random.randint(key_hot, (ROWS,), 0, hot_span)
    use_hot = jax.random.randint(key_pick, (ROWS,), 0, 2) == 1
    position = jnp.arange(ROWS) % TOKENS
    first_expert = jnp.where(use_hot, start_hot, start_any)
    first_expert = jnp.where(position <= SLOTS, 0, first_expert)
    choice = (first_expert[:, None] + spacing * jnp.arange(TOP_K)[None, :]) % EXPERTS
    choice = choice.astype(jnp.int32)

    def device_slots(dev_choice):
        flat_ids = dev_choice.reshape(-1)
        onehot = (flat_ids[:, None] == jnp.arange(EXPERTS)[None, :]).astype(jnp.int32)
        rank_pos = jnp.sum(jnp.cumsum(onehot, axis=0) * onehot, axis=1) - 1
        return jnp.where(rank_pos < SLOTS, rank_pos, -1).reshape(TOKENS, TOP_K)

    slot_ids = lax.map(device_slots, choice.reshape(GROUP, TOKENS, TOP_K))
    return choice, slot_ids.reshape(ROWS, TOP_K).astype(jnp.int32)


def setup_inputs(seed: int = 0, part: int = 0) -> dict:
    base_key = jax.random.key(seed)
    part_key = jax.random.fold_in(base_key, part)
    part_keys = jax.random.split(part_key, 6)
    shared_keys = jax.random.split(base_key, 9)
    scale_in = MODEL_DIM ** -0.5
    scale_ffn = FFN_DIM ** -0.5
    experts_a, slots_a = draw_routing(part_keys[1])
    experts_b, slots_b = draw_routing(part_keys[4])
    return {
        "tokens_a": jax.random.normal(part_keys[0], (ROWS, MODEL_DIM), jnp.float32).astype(jnp.bfloat16),
        "experts_a": experts_a,
        "slots_a": slots_a,
        "gates_a": jax.random.uniform(part_keys[2], (ROWS, TOP_K), jnp.float32, 0.5, 1.5).astype(jnp.bfloat16),
        "tokens_b": jax.random.normal(part_keys[3], (ROWS, MODEL_DIM), jnp.float32).astype(jnp.bfloat16),
        "experts_b": experts_b,
        "slots_b": slots_b,
        "gates_b": jax.random.uniform(part_keys[5], (ROWS, TOP_K), jnp.float32, 0.5, 1.5).astype(jnp.bfloat16),
        "attn_gain": (1.0 + 0.3 * jax.random.normal(shared_keys[0], (MODEL_DIM,), jnp.float32)).astype(jnp.bfloat16),
        "w_query": (1.5 * scale_in * jax.random.normal(shared_keys[1], (MODEL_DIM, HEADS, HEAD_DIM), jnp.float32)).astype(jnp.bfloat16),
        "w_key": (1.5 * scale_in * jax.random.normal(shared_keys[2], (MODEL_DIM, HEADS, HEAD_DIM), jnp.float32)).astype(jnp.bfloat16),
        "w_value": (scale_in * jax.random.normal(shared_keys[3], (MODEL_DIM, HEADS, HEAD_DIM), jnp.float32)).astype(jnp.bfloat16),
        "w_out": (scale_in * jax.random.normal(shared_keys[4], (HEADS, HEAD_DIM, MODEL_DIM), jnp.float32)).astype(jnp.bfloat16),
        "moe_gain": (1.0 + 0.3 * jax.random.normal(shared_keys[5], (MODEL_DIM,), jnp.float32)).astype(jnp.bfloat16),
        "w_gate": (scale_in * jax.random.normal(shared_keys[6], (EXPERTS, MODEL_DIM, FFN_DIM), jnp.float32)).astype(jnp.bfloat16),
        "w_up": (scale_in * jax.random.normal(shared_keys[7], (EXPERTS, MODEL_DIM, FFN_DIM), jnp.float32)).astype(jnp.bfloat16),
        "w_down": (scale_ffn * jax.random.normal(shared_keys[8], (EXPERTS, FFN_DIM, MODEL_DIM), jnp.float32)).astype(jnp.bfloat16),
    }


def rms_norm(rows, gain_vec):
    rows_f = rows.astype(jnp.float32)
    inv_rms = lax.rsqrt(jnp.mean(rows_f * rows_f, axis=-1, keepdims=True) + NORM_EPS)
    return (rows_f * inv_rms * gain_vec.astype(jnp.float32)).astype(jnp.bfloat16)


def attention_block(sequence, attn_gain, w_query, w_key, w_value, w_out):
    normed = rms_norm(sequence, attn_gain).astype(jnp.float32)
    query = jnp.einsum("td,dhe->the", normed, w_query.astype(jnp.float32)).astype(jnp.bfloat16)
    keys = jnp.einsum("td,dhe->the", normed, w_key.astype(jnp.float32)).astype(jnp.bfloat16)
    values = jnp.einsum("td,dhe->the", normed, w_value.astype(jnp.float32)).astype(jnp.bfloat16)
    scores = jnp.einsum("qhe,khe->hqk", query.astype(jnp.float32), keys.astype(jnp.float32)) * (HEAD_DIM ** -0.5)
    causal = jnp.arange(TOKENS)[:, None] >= jnp.arange(TOKENS)[None, :]
    scores = jnp.where(causal[None, :, :], scores, MASK_VALUE)
    attn_prob = jax.nn.softmax(scores, axis=-1).astype(jnp.bfloat16)
    context = jnp.einsum("hqk,khe->qhe", attn_prob.astype(jnp.float32), values.astype(jnp.float32)).astype(jnp.bfloat16)
    attn_out = jnp.einsum("qhe,hed->qd", context.astype(jnp.float32), w_out.astype(jnp.float32))
    return (sequence.astype(jnp.float32) + attn_out).astype(jnp.bfloat16)


def moe_layer(tokens, experts, slots, gates, attn_gain, w_query, w_key, w_value, w_out, moe_gain, w_gate, w_up, w_down):
    residual = lax.map(lambda sequence: attention_block(sequence, attn_gain, w_query, w_key, w_value, w_out), tokens.reshape(GROUP, TOKENS, MODEL_DIM))
    normed = rms_norm(residual, moe_gain).reshape(ROWS, MODEL_DIM)
    row_ids = jnp.arange(ROWS, dtype=jnp.int32)
    owner = row_ids // TOKENS
    buffer_rows = EXPERTS * GROUP * SLOTS
    dest_row = jnp.where(slots >= 0, experts * (GROUP * SLOTS) + owner[:, None] * SLOTS + slots, buffer_rows)
    token_of = jnp.broadcast_to(row_ids[:, None], (ROWS, TOP_K)).reshape(-1)
    source = jnp.full((buffer_rows,), ROWS, jnp.int32).at[dest_row.reshape(-1)].set(token_of, mode="drop")

    def expert_ffn(operands):
        expert_source, gate_w, up_w, down_w = operands
        rows_in = jnp.take(normed, expert_source, axis=0, mode="fill", fill_value=0)
        gate_act = jnp.dot(rows_in, gate_w, preferred_element_type=jnp.float32)
        up_act = jnp.dot(rows_in, up_w, preferred_element_type=jnp.float32)
        hidden = (jax.nn.silu(gate_act) * up_act).astype(jnp.bfloat16)
        return jnp.dot(hidden, down_w, preferred_element_type=jnp.float32).astype(jnp.bfloat16)

    expert_out = lax.map(expert_ffn, (source.reshape(EXPERTS, GROUP * SLOTS), w_gate, w_up, w_down)).reshape(buffer_rows, MODEL_DIM)

    def combine(operands):
        dev_resid, dev_dest, dev_gates = operands
        picked = jnp.take(expert_out, dev_dest, axis=0, mode="fill", fill_value=0).reshape(TOKENS, TOP_K, MODEL_DIM)
        mixed_sum = jnp.einsum("tk,tkd->td", dev_gates.astype(jnp.float32), picked.astype(jnp.float32))
        return (dev_resid.astype(jnp.float32) + mixed_sum).astype(jnp.bfloat16)

    mixed_rows = lax.map(combine, (residual, dest_row.reshape(GROUP, TOKENS * TOP_K), gates.reshape(GROUP, TOKENS, TOP_K)))
    return mixed_rows.reshape(ROWS, MODEL_DIM)


def reference(tokens_a, experts_a, slots_a, gates_a, tokens_b, experts_b, slots_b, gates_b, attn_gain, w_query, w_key, w_value, w_out, moe_gain, w_gate, w_up, w_down):
    out_a = moe_layer(tokens_a, experts_a, slots_a, gates_a, attn_gain, w_query, w_key, w_value, w_out, moe_gain, w_gate, w_up, w_down)
    out_b = moe_layer(tokens_b, experts_b, slots_b, gates_b, attn_gain, w_query, w_key, w_value, w_out, moe_gain, w_gate, w_up, w_down)
    return (out_a, out_b)
```

```python
import functools

import jax
import jax.numpy as jnp
from jax import lax
from jax.experimental import pallas as pl
from jax.experimental.pallas import tpu as pltpu
from jax.sharding import PartitionSpec as P

NORM_EPS = 1e-6
MASK_VALUE = -1e30
LANES = 128
PIECES = 1
MESH = pl.DeviceIdType.MESH
NT = (((1,), (1,)), ((), ()))
TN = (((0,), (0,)), ((), ()))
F32 = jnp.float32
BF16 = jnp.bfloat16


def layer_kernel(
    group,
    tok_a, exp_a, slot_a, gate_a, tok_b, exp_b, slot_b, gate_b, attn_gain, wq_h, wk_h, wv_h, wo_h, moe_gain, wg_h, wu_h, wd_h,
    out_a, out_b,
    x_ref, exp_ref, slot_ref, gate_ref, again_ref, mgain_ref, wq, wk, wv, wo, wg, wu, wd,
    a_ref, q_ref, k_ref, v_ref, c_ref, h_ref, usend, uown, ulr, ufar, sel_ref, wbuf, hid_ref,
    part, pfar, pown, rbuf, fin, ownr, out_ref,
    lsem, ssem, wrecv, orecv, agrecv, rsrecv, finrecv,
):
    seq, dim = tok_a.shape
    both = 2 * seq
    blocks = dim // LANES
    urows = blocks * seq
    local = wg_h.shape[0]
    experts = 2 * local
    ffn = wg_h.shape[2]
    top_k = exp_a.shape[0]
    chips = group // 2
    half = chips // 2
    gw_rows = local * group // 2

    me = lax.axis_index("ep")
    z = lax.div(me, 2)
    core = lax.rem(me, 2)
    other = 1 - core
    sibling = 2 * z + other
    right = lax.rem(z + 1, chips)
    left = lax.rem(z + chips - 1, chips)
    toward = (right, left)

    barrier = pltpu.get_barrier_semaphore()
    for peer in (2 * left, 2 * left + 1, 2 * right, 2 * right + 1, sibling):
        pl.semaphore_signal(barrier, inc=1, device_id={"ep": peer}, device_id_type=MESH)

    sends = []

    def local_copy(i, src, dst):
        copy = pltpu.make_async_copy(src, dst, lsem.at[i])
        copy.start()
        return copy

    def remote(src, dst, rsem, peer):
        copy = pltpu.make_async_remote_copy(
            src_ref=src, dst_ref=dst, send_sem=ssem.at[len(sends)], recv_sem=rsem, device_id={"ep": peer}, device_id_type=MESH
        )
        copy.start()
        sends.append(copy)

    def arrived(dst, rsem):
        pltpu.make_async_remote_copy(
            src_ref=dst, dst_ref=dst, send_sem=ssem.at[0], recv_sem=rsem, device_id={"ep": sibling}, device_id_type=MESH
        ).wait_recv()

    small = [
        local_copy(0, tok_a, x_ref.at[pl.ds(0, seq)]),
        local_copy(1, tok_b, x_ref.at[pl.ds(seq, seq)]),
        local_copy(2, attn_gain, again_ref),
        local_copy(3, moe_gain, mgain_ref),
    ]
    loads = [local_copy(4, wq_h, wq), local_copy(5, wk_h, wk), local_copy(6, wv_h, wv)]
    routes = [
        local_copy(7, exp_a, exp_ref.at[0]),
        local_copy(8, exp_b, exp_ref.at[1]),
        local_copy(9, slot_a, slot_ref.at[0]),
        local_copy(10, slot_b, slot_ref.at[1]),
        local_copy(11, gate_a, gate_ref.at[0]),
        local_copy(12, gate_b, gate_ref.at[1]),
    ]
    load_out = local_copy(13, wo_h, wo)
    mine = pl.ds(0, local)
    theirs = pl.ds(local, local)
    ffn_loads = [local_copy(14, wg_h, wg.at[mine]), local_copy(15, wu_h, wu.at[mine]), local_copy(16, wd_h, wd.at[mine])]

    def rms(src_ref, gain_ref, put):
        gain = gain_ref[...].astype(F32)

        def strip(i, carry):
            rows = pl.ds(pl.multiple_of(i * 16, 16), 16)
            xs = src_ref[rows, :].astype(F32)
            inv = lax.rsqrt(jnp.mean(xs * xs, axis=-1, keepdims=True) + NORM_EPS)
            for j in range(blocks):
                put(i, j, (xs[:, j * LANES:(j + 1) * LANES] * inv * gain[j:j + 1, :]).astype(BF16))
            return carry

        lax.fori_loop(0, both // 16, strip, 0)

    for copy in small:
        copy.wait()

    def put_a(i, j, val):
        a_ref[pl.ds(pl.multiple_of(i * 16, 16), 16), j * LANES:(j + 1) * LANES] = val

    rms(x_ref, again_ref, put_a)
    wide = 256
    for load, w, dst in zip(loads, (wq, wk, wv), (q_ref, k_ref, v_ref)):
        load.wait()
        for n in range(dim // wide):
            cols = slice(n * wide, (n + 1) * wide)
            dst[:, cols] = lax.dot_general(a_ref[...], w[cols, :], NT, preferred_element_type=F32).astype(BF16)

    pl.semaphore_wait(barrier, 5)
    remote(wg_h, wg.at[theirs], wrecv.at[0], sibling)
    remote(wu_h, wu.at[theirs], wrecv.at[1], sibling)
    remote(wd_h, wd.at[theirs], wrecv.at[2], sibling)

    row = lax.broadcasted_iota(jnp.int32, (2 * both, both), 0)
    col = lax.broadcasted_iota(jnp.int32, (2 * both, both), 1)
    row = jnp.where(row >= both, row - both, row)
    allowed = (row >= col) & ((row >= seq) == (col >= seq))
    lane = lax.broadcasted_iota(jnp.int32, (both, LANES), 1)
    head_dim = LANES // 2
    scale = head_dim ** -0.5
    for p in range(dim // LANES):
        cols = slice(p * LANES, (p + 1) * LANES)
        qp = q_ref[:, cols].astype(F32)
        vp = v_ref[:, cols].astype(F32)
        low = lane < head_dim
        qq = jnp.concatenate([jnp.where(low, qp, 0.0), jnp.where(low, 0.0, qp)], axis=0).astype(BF16)
        vv = jnp.concatenate([jnp.where(low, vp, 0.0), jnp.where(low, 0.0, vp)], axis=0).astype(BF16)
        s = lax.dot_general(qq, k_ref[:, cols], NT, preferred_element_type=F32) * scale
        s = jnp.where(allowed, s, MASK_VALUE)
        e = jnp.exp(s - jnp.max(s, axis=-1, keepdims=True))
        prob = (e / jnp.sum(e, axis=-1, keepdims=True)).astype(BF16)
        pp = jnp.concatenate([prob[:both], prob[both:]], axis=1)
        c_ref[:, cols] = jnp.dot(pp, vv, preferred_element_type=F32).astype(BF16)

    load_out.wait()
    for n in range(dim // wide):
        cols = slice(n * wide, (n + 1) * wide)
        res = jnp.dot(c_ref[...], wo[:, cols], preferred_element_type=F32)
        h_ref[:, cols] = (x_ref[:, cols].astype(F32) + res).astype(BF16)

    for copy in routes:
        copy.wait()
    eid = lax.broadcasted_iota(jnp.int32, (gw_rows, LANES), 0)
    eid = jnp.where(lax.broadcasted_iota(jnp.int32, (gw_rows, LANES), 1) >= seq, eid + gw_rows, eid)
    for b in range(2):
        ids = jnp.where(slot_ref[b] >= 0, exp_ref[b], -1)
        ids = jnp.concatenate([ids, ids], axis=1)
        gts = gate_ref[b].astype(F32)
        gts = jnp.concatenate([gts, gts], axis=1)
        gw = jnp.zeros((gw_rows, LANES), F32)
        for j in range(top_k):
            gw = gw + jnp.where(ids[j:j + 1, :] == eid, gts[j:j + 1, :], 0.0)
        usend[b, pl.ds(urows, gw_rows), :] = gw.astype(BF16)

    def put_u(i, j, val):
        b = lax.div(i, seq // 16)
        r = lax.rem(i, seq // 16) * 16
        usend[b, pl.ds(pl.multiple_of(j * seq + r, 16), 16), :] = val

    rms(h_ref, mgain_ref, put_u)

    for b in range(2):
        for d in range(2):
            remote(usend.at[b], ulr.at[0, core, d], agrecv.at[0, core, d], 2 * toward[d] + b)
    remote(usend.at[other], uown, orecv.at[0], sibling)

    first = lax.rem(experts * z, gw_rows)
    upper = (experts * z) // gw_rows
    sel_row = lax.broadcasted_iota(jnp.int32, (gw_rows, experts * LANES), 0)
    sel_slot = lax.div(lax.broadcasted_iota(jnp.int32, (gw_rows, experts * LANES), 1), LANES)
    wanted = first + lax.rem(local * core + sel_slot, experts)
    sel_ref[...] = jnp.where(sel_row == wanted, 1.0, 0.0).astype(BF16)

    def gates_of(sub):
        packed = sub[pl.ds(urows, gw_rows), :]
        w = lax.dot_general(packed, sel_ref[...], TN, preferred_element_type=F32)
        return jnp.where(upper == 1, w[seq:], w[:seq])

    def expert_pair(sub0, sub1, dst):
        for i, sub in enumerate((sub0, sub1)):
            w = gates_of(sub)
            for k in range(experts):
                wbuf[k, i * seq:(i + 1) * seq, :] = w[:, k * LANES:(k + 1) * LANES]
        dst[...] = jnp.zeros(dst.shape, F32)

        def one(k, carry):
            rows = jnp.concatenate(
                [jnp.concatenate([sub[j * seq:(j + 1) * seq, :] for j in range(blocks)], axis=1) for sub in (sub0, sub1)], axis=0
            )
            for n in range(ffn // wide):
                cols = slice(n * wide, (n + 1) * wide)
                g = jnp.dot(rows, wg[k, :, cols], preferred_element_type=F32)
                up = jnp.dot(rows, wu[k, :, cols], preferred_element_type=F32)
                hid_ref[:, cols] = (jax.nn.silu(g) * up).astype(BF16)
            w = wbuf[k]
            for n in range(dim // wide):
                o = jnp.dot(hid_ref[...], wd[k, :, n * wide:(n + 1) * wide], preferred_element_type=F32)
                o = o.astype(BF16).astype(F32)
                for m in range(wide // LANES):
                    cols = slice(n * wide + m * LANES, n * wide + (m + 1) * LANES)
                    dst[:, cols] += jnp.where(w > 0.0, w * o[:, m * LANES:(m + 1) * LANES], 0.0)
            return carry

        lax.fori_loop(0, experts, one, 0)

    size = seq // PIECES

    def partial_of(d, c, k, g):
        if k == half:
            return pfar.at[pl.ds(c * seq + g * size, size)]
        return part.at[k - 1, c, pl.ds((1 - d) * seq + g * size, size)]

    def pass_on(d, c, k):
        for g in range(PIECES):
            src = partial_of(d, c, k, g)
            if k > 1:
                dst = rbuf.at[d, k - 2, c, pl.ds(g * size, size)]
                remote(src, dst, rsrecv.at[d, k - 2, c, g], 2 * toward[d] + core)
            else:
                dst = fin.at[core, d, pl.ds(g * size, size)]
                remote(src, dst, finrecv.at[core, d, g], 2 * toward[d] + c)

    def add_and_pass(d, c, k):
        for g in range(PIECES):
            got = rbuf.at[d, k - 1, c, pl.ds(g * size, size)]
            arrived(got, rsrecv.at[d, k - 1, c, g])
            mine_k = partial_of(d, c, k, g)
            mine_k[...] += got[...]
        pass_on(d, c, k)

    for h in range(half - 1):
        for c in range(2):
            for d in range(2):
                arrived(ulr.at[h, c, d], agrecv.at[h, c, d])
                if h + 1 < half - 1:
                    remote(ulr.at[h, c, d], ulr.at[h + 1, c, d], agrecv.at[h + 1, c, d], 2 * toward[d] + core)
                elif c == d:
                    remote(ulr.at[h, c, d], ufar.at[c], agrecv.at[h + 1, c, d], 2 * toward[d] + core)
            if h == 0 and c == 0:
                for copy in ffn_loads:
                    copy.wait()
                arrived(wg.at[theirs], wrecv.at[0])
                arrived(wu.at[theirs], wrecv.at[1])
                arrived(wd.at[theirs], wrecv.at[2])
            expert_pair(ulr.at[h, c, 0], ulr.at[h, c, 1], part.at[h, c])
    for d in range(2):
        pass_on(d, 1 - d, half - 1)
    for c in range(2):
        arrived(ufar.at[c], agrecv.at[half - 1, c, c])
    expert_pair(ufar.at[0], ufar.at[1], pfar)
    for d in range(2):
        pass_on(d, d, half)

    arrived(uown, orecv.at[0])
    expert_pair(usend.at[core], uown, pown)
    remote(pown.at[pl.ds(seq, seq)], ownr, orecv.at[1], sibling)

    for r in range(half - 1):
        for d in range(2):
            if half - 2 - r >= 1:
                add_and_pass(d, 1 - d, half - 2 - r)
        for d in range(2):
            add_and_pass(d, d, half - 1 - r)

    arrived(ownr, orecv.at[1])
    for b in range(2):
        for d in range(2):
            for g in range(PIECES):
                arrived(fin.at[b, d, pl.ds(g * size, size)], finrecv.at[b, d, g])
    for b, own in ((core, pown.at[pl.ds(0, seq)]), (other, ownr)):
        hrow = pl.ds(pl.multiple_of(b * seq, seq), seq)
        out_ref[b] = (h_ref[hrow, :].astype(F32) + (own[...] + (fin[b, 0] + fin[b, 1]))).astype(BF16)
    outs = [local_copy(0, out_ref.at[0], out_a), local_copy(1, out_ref.at[1], out_b)]
    for copy in outs:
        copy.wait()
    for copy in sends:
        copy.wait_send()


def solution(mesh):
    group = mesh.shape["ep"]
    row_spec = P(("dp", "ep"), None)
    full_spec = P(None, None, None)
    gain_spec = P(None)
    expert_spec = P("ep", None, None)
    in_specs = (row_spec,) * 8 + (gain_spec, full_spec, full_spec, full_spec, full_spec, gain_spec, expert_spec, expert_spec, expert_spec)

    def device_fn(tokens_a, experts_a, slots_a, gates_a, tokens_b, experts_b, slots_b, gates_b, attn_gain, w_query, w_key, w_value, w_out, moe_gain, w_gate, w_up, w_down):
        seq, dim = tokens_a.shape
        top_k = experts_a.shape[1]
        heads, head_dim = w_query.shape[1:]
        local, _, ffn = w_gate.shape
        half = group // 4
        both = 2 * seq
        urows = dim // LANES * seq
        urows_all = urows + local * group // 2

        def project(w):
            return w.transpose(1, 2, 0).reshape(heads * head_dim, dim)

        args = (
            tokens_a, experts_a.T, slots_a.T, gates_a.T, tokens_b, experts_b.T, slots_b.T, gates_b.T,
            attn_gain.reshape(dim // LANES, LANES), project(w_query), project(w_key), project(w_value),
            w_out.reshape(heads * head_dim, dim), moe_gain.reshape(dim // LANES, LANES), w_gate, w_up, w_down,
        )
        vmem = pltpu.VMEM
        scratch = [
            vmem((both, dim), BF16),
            vmem((2, top_k, seq), jnp.int32),
            vmem((2, top_k, seq), jnp.int32),
            vmem((2, top_k, seq), BF16),
            vmem((dim // LANES, LANES), BF16),
            vmem((dim // LANES, LANES), BF16),
            vmem((heads * head_dim, dim), BF16),
            vmem((heads * head_dim, dim), BF16),
            vmem((heads * head_dim, dim), BF16),
            vmem((heads * head_dim, dim), BF16),
            vmem((2 * local, dim, ffn), BF16),
            vmem((2 * local, dim, ffn), BF16),
            vmem((2 * local, ffn, dim), BF16),
            vmem((both, dim), BF16),
            vmem((both, dim), BF16),
            vmem((both, dim), BF16),
            vmem((both, dim), BF16),
            vmem((both, dim), BF16),
            vmem((both, dim), BF16),
            vmem((2, urows_all, LANES), BF16),
            vmem((urows_all, LANES), BF16),
            vmem((half - 1, 2, 2, urows_all, LANES), BF16),
            vmem((2, urows_all, LANES), BF16),
            vmem((local * group // 2, 2 * local * LANES), BF16),
            vmem((2 * local, both, LANES), F32),
            vmem((both, ffn), BF16),
            vmem((half - 1, 2, both, dim), F32),
            vmem((both, dim), F32),
            vmem((both, dim), F32),
            vmem((2, half - 1, 2, seq, dim), F32),
            vmem((2, 2, seq, dim), F32),
            vmem((seq, dim), F32),
            vmem((2, seq, dim), BF16),
            pltpu.SemaphoreType.DMA((17,)),
            pltpu.SemaphoreType.DMA((9 + 4 * (half - 2) + 2 + 1 + (2 * half - 1) * 2 * PIECES,)),
            pltpu.SemaphoreType.DMA((3,)),
            pltpu.SemaphoreType.DMA((2,)),
            pltpu.SemaphoreType.DMA((half, 2, 2)),
            pltpu.SemaphoreType.DMA((2, half - 1, 2, PIECES)),
            pltpu.SemaphoreType.DMA((2, 2, PIECES)),
        ]
        rows_all = group * seq
        return pl.pallas_call(
            functools.partial(layer_kernel, group),
            name="layer",
            out_shape=[jax.ShapeDtypeStruct((seq, dim), BF16)] * 2,
            in_specs=[pl.BlockSpec(memory_space=pl.ANY)] * len(args),
            out_specs=[pl.BlockSpec(memory_space=pl.ANY)] * 2,
            scratch_shapes=scratch,
            compiler_params=pltpu.CompilerParams(collective_id=0, has_side_effects=True, vmem_limit_bytes=60 * 1024 * 1024),
            cost_estimate=pl.CostEstimate(
                flops=rows_all * 6 * 2 * local * dim * ffn + both * 8 * dim * dim, bytes_accessed=2 * dim * (4 * dim + 3 * local * ffn), transcendentals=0
            ),
        )(*args)

    return jax.shard_map(device_fn, mesh=mesh, in_specs=in_specs, out_specs=(row_spec, row_spec), check_vma=False)
```

```python
import functools

import jax
import jax.numpy as jnp
from jax import lax
from jax.experimental import pallas as pl
from jax.experimental.pallas import tpu as pltpu
from jax.sharding import PartitionSpec as P

NORM_EPS = 1e-6
MASK_VALUE = -1e30
LANES = 128
PIECES = 2
MESH = pl.DeviceIdType.MESH
NT = (((1,), (1,)), ((), ()))
TN = (((0,), (0,)), ((), ()))
F32 = jnp.float32
BF16 = jnp.bfloat16


def layer_kernel(
    group,
    tok_a, exp_a, slot_a, gate_a, tok_b, exp_b, slot_b, gate_b, attn_gain, wq_h, wk_h, wv_h, wo_h, moe_gain, wg_h, wu_h, wd_h,
    out,
    x_ref, exp_ref, slot_ref, gate_ref, again_ref, mgain_ref, wq, wk, wv, wo, wg, wu, wd,
    a_ref, q_ref, k_ref, v_ref, c_ref, h_ref, usend, uown, ulr, ufar, sel_ref, wbuf, hid_ref,
    part, pfar, pown, rbuf, fin, ownr, out_ref,
    lsem, ssem, wrecv, orecv, agrecv, rsrecv, finrecv,
):
    seq, dim = tok_a.shape
    both = 2 * seq
    blocks = dim // LANES
    urows = blocks * seq
    local = wg_h.shape[0]
    experts = 2 * local
    ffn = wg_h.shape[2]
    top_k = exp_a.shape[0]
    chips = group // 2
    half = chips // 2
    gw_rows = local * group // 2

    me = lax.axis_index("ep")
    z = lax.div(me, 2)
    core = lax.rem(me, 2)
    other = 1 - core
    sibling = 2 * z + other
    right = lax.rem(z + 1, chips)
    left = lax.rem(z + chips - 1, chips)
    toward = (right, left)

    barrier = pltpu.get_barrier_semaphore()
    for peer in (2 * left, 2 * left + 1, 2 * right, 2 * right + 1, sibling):
        pl.semaphore_signal(barrier, inc=1, device_id={"ep": peer}, device_id_type=MESH)

    sends = []

    def local_copy(i, src, dst):
        copy = pltpu.make_async_copy(src, dst, lsem.at[i])
        copy.start()
        return copy

    def remote(src, dst, rsem, peer):
        copy = pltpu.make_async_remote_copy(
            src_ref=src, dst_ref=dst, send_sem=ssem.at[len(sends)], recv_sem=rsem, device_id={"ep": peer}, device_id_type=MESH
        )
        copy.start()
        sends.append(copy)

    def arrived(dst, rsem):
        pltpu.make_async_remote_copy(
            src_ref=dst, dst_ref=dst, send_sem=ssem.at[0], recv_sem=rsem, device_id={"ep": sibling}, device_id_type=MESH
        ).wait_recv()

    small = [
        local_copy(0, tok_a, x_ref.at[pl.ds(0, seq)]),
        local_copy(1, tok_b, x_ref.at[pl.ds(seq, seq)]),
        local_copy(2, attn_gain, again_ref),
        local_copy(3, moe_gain, mgain_ref),
    ]
    parts = [pl.ds(i * (dim // 4), dim // 4) for i in range(4)]
    loads = [[local_copy(17 + i, wq_h.at[rows], wq.at[rows]) for i, rows in enumerate(parts)]]
    loads += [[local_copy(5, wk_h, wk)], [local_copy(6, wv_h, wv)]]
    routes = [
        local_copy(7, exp_a, exp_ref.at[0]),
        local_copy(8, exp_b, exp_ref.at[1]),
        local_copy(9, slot_a, slot_ref.at[0]),
        local_copy(10, slot_b, slot_ref.at[1]),
        local_copy(11, gate_a, gate_ref.at[0]),
        local_copy(12, gate_b, gate_ref.at[1]),
    ]
    load_out = local_copy(13, wo_h, wo)
    mine = pl.ds(0, local)
    theirs = pl.ds(local, local)
    ffn_loads = [local_copy(14, wg_h, wg.at[mine]), local_copy(15, wu_h, wu.at[mine]), local_copy(16, wd_h, wd.at[mine])]

    def rms(src_ref, gain_ref, put):
        gain = gain_ref[...].astype(F32)

        def strip(i, carry):
            rows = pl.ds(pl.multiple_of(i * 16, 16), 16)
            xs = src_ref[rows, :].astype(F32)
            inv = lax.rsqrt(jnp.mean(xs * xs, axis=-1, keepdims=True) + NORM_EPS)
            for j in range(blocks):
                put(i, j, (xs[:, j * LANES:(j + 1) * LANES] * inv * gain[j:j + 1, :]).astype(BF16))
            return carry

        lax.fori_loop(0, both // 16, strip, 0, unroll=True)

    pl.semaphore_wait(barrier, 5)
    remote(wg_h, wg.at[theirs], wrecv.at[0], sibling)
    remote(wu_h, wu.at[theirs], wrecv.at[1], sibling)
    remote(wd_h, wd.at[theirs], wrecv.at[2], sibling)

    for copy in small:
        copy.wait()

    def put_a(i, j, val):
        a_ref[pl.ds(pl.multiple_of(i * 16, 16), 16), j * LANES:(j + 1) * LANES] = val

    rms(x_ref, again_ref, put_a)
    wide = 256
    for load, w, dst in zip(loads, (wq, wk, wv), (q_ref, k_ref, v_ref)):
        for n in range(dim // LANES):
            if n % (dim // LANES // len(load)) == 0:
                load[n // (dim // LANES // len(load))].wait()
            cols = slice(n * LANES, (n + 1) * LANES)
            dst[:, cols] = lax.dot_general(a_ref[...], w[cols, :], NT, preferred_element_type=F32).astype(BF16)

    row = lax.broadcasted_iota(jnp.int32, (2 * both, both), 0)
    col = lax.broadcasted_iota(jnp.int32, (2 * both, both), 1)
    row = jnp.where(row >= both, row - both, row)
    allowed = (row >= col) & ((row >= seq) == (col >= seq))
    lane = lax.broadcasted_iota(jnp.int32, (both, LANES), 1)
    head_dim = LANES // 2
    scale = head_dim ** -0.5
    for p in range(dim // LANES):
        cols = slice(p * LANES, (p + 1) * LANES)
        qp = q_ref[:, cols].astype(F32)
        vp = v_ref[:, cols].astype(F32)
        low = lane < head_dim
        qq = jnp.concatenate([jnp.where(low, qp, 0.0), jnp.where(low, 0.0, qp)], axis=0).astype(BF16)
        vv = jnp.concatenate([jnp.where(low, vp, 0.0), jnp.where(low, 0.0, vp)], axis=0).astype(BF16)
        s = lax.dot_general(qq, k_ref[:, cols], NT, preferred_element_type=F32) * scale
        s = jnp.where(allowed, s, MASK_VALUE)
        e = jnp.exp(s - jnp.max(s, axis=-1, keepdims=True))
        prob = (e / jnp.sum(e, axis=-1, keepdims=True)).astype(BF16)
        pp = jnp.concatenate([prob[:both], prob[both:]], axis=1)
        c_ref[:, cols] = jnp.dot(pp, vv, preferred_element_type=F32).astype(BF16)

    load_out.wait()
    for n in range(dim // wide):
        cols = slice(n * wide, (n + 1) * wide)
        res = jnp.dot(c_ref[...], wo[:, cols], preferred_element_type=F32)
        h_ref[:, cols] = (x_ref[:, cols].astype(F32) + res).astype(BF16)

    for copy in routes:
        copy.wait()
    eid = lax.broadcasted_iota(jnp.int32, (gw_rows, LANES), 0)
    eid = jnp.where(lax.broadcasted_iota(jnp.int32, (gw_rows, LANES), 1) >= seq, eid + gw_rows, eid)
    for b in range(2):
        ids = jnp.where(slot_ref[b] >= 0, exp_ref[b], -1)
        ids = jnp.concatenate([ids, ids], axis=1)
        gts = gate_ref[b].astype(F32)
        gts = jnp.concatenate([gts, gts], axis=1)
        gw = jnp.zeros((gw_rows, LANES), F32)
        for j in range(top_k):
            gw = gw + jnp.where(ids[j:j + 1, :] == eid, gts[j:j + 1, :], 0.0)
        usend[b, pl.ds(urows, gw_rows), :] = gw.astype(BF16)

    def put_u(i, j, val):
        b = lax.div(i, seq // 16)
        r = lax.rem(i, seq // 16) * 16
        usend[b, pl.ds(pl.multiple_of(j * seq + r, 16), 16), :] = val

    rms(h_ref, mgain_ref, put_u)

    def first_hop(b, d):
        remote(usend.at[b], ulr.at[0, core, d], agrecv.at[0, core, d], 2 * jnp.where(d == 0, right, left) + b)

    remote(usend.at[other], uown, orecv.at[0], sibling)
    first_hop(0, core)
    first_hop(1, core)
    first = lax.rem(experts * z, gw_rows)
    upper = (experts * z) // gw_rows
    sel_row = lax.broadcasted_iota(jnp.int32, (gw_rows, experts * LANES), 0)
    sel_slot = lax.div(lax.broadcasted_iota(jnp.int32, (gw_rows, experts * LANES), 1), LANES)
    wanted = first + lax.rem(local * core + sel_slot, experts)
    sel_ref[...] = jnp.where(sel_row == wanted, 1.0, 0.0).astype(BF16)
    first_hop(0, other)
    first_hop(1, other)

    def gates_of(sub):
        packed = sub[pl.ds(urows, gw_rows), :]
        w = lax.dot_general(packed, sel_ref[...], TN, preferred_element_type=F32)
        return jnp.where(upper == 1, w[seq:], w[:seq])

    def expert_pair(sub0, sub1, dst):
        for i, sub in enumerate((sub0, sub1)):
            w = gates_of(sub)
            for k in range(experts):
                wbuf[k, i * seq:(i + 1) * seq, :] = w[:, k * LANES:(k + 1) * LANES]
        rows = jnp.concatenate(
            [jnp.concatenate([sub[j * seq:(j + 1) * seq, :] for j in range(blocks)], axis=1) for sub in (sub0, sub1)], axis=0
        )
        for k in range(experts):
            for n in range(ffn // wide):
                cols = slice(n * wide, (n + 1) * wide)
                g = jnp.dot(rows, wg[k, :, cols], preferred_element_type=F32)
                up = jnp.dot(rows, wu[k, :, cols], preferred_element_type=F32)
                hid_ref[k, :, cols] = (jax.nn.silu(g) * up).astype(BF16)
        for n in range(dim // wide):
            total = None
            for k in range(experts):
                o = jnp.dot(hid_ref[k], wd[k, :, n * wide:(n + 1) * wide], preferred_element_type=F32)
                o = o.astype(BF16).astype(F32)
                w = wbuf[k]
                term = jnp.concatenate(
                    [jnp.where(w > 0.0, w * o[:, m * LANES:(m + 1) * LANES], 0.0) for m in range(wide // LANES)], axis=1
                )
                total = term if total is None else total + term
            dst[:, n * wide:(n + 1) * wide] = total

    size = seq // PIECES

    def partial_of(d, c, k, g):
        if k == half:
            return pfar.at[pl.ds(c * seq + g * size, size)]
        came = 1 - d
        return part.at[k - 1, 0 if c == came else 1, pl.ds(came * seq + g * size, size)]

    def pass_on(d, c, k, g):
        src = partial_of(d, c, k, g)
        if k > 1:
            dst = rbuf.at[d, k - 2, c, pl.ds(g * size, size)]
            remote(src, dst, rsrecv.at[d, k - 2, c, g], 2 * toward[d] + core)
        else:
            dst = fin.at[core, d, pl.ds(g * size, size)]
            remote(src, dst, finrecv.at[core, d, g], 2 * toward[d] + c)

    def add_and_pass(d, c, k, g):
        got = rbuf.at[d, k - 1, c, pl.ds(g * size, size)]
        arrived(got, rsrecv.at[d, k - 1, c, g])
        mine_k = partial_of(d, c, k, g)
        mine_k[...] += got[...]
        pass_on(d, c, k, g)

    both_ways = [(d, g) for g in range(PIECES) for d in range(2)]

    for h in range(half - 1):
        for first_set in (True, False):
            for d in range(2):
                c = d if first_set else 1 - d
                arrived(ulr.at[h, c, d], agrecv.at[h, c, d])
                if h + 1 < half - 1:
                    remote(ulr.at[h, c, d], ulr.at[h + 1, c, d], agrecv.at[h + 1, c, d], 2 * toward[d] + core)
                elif first_set:
                    remote(ulr.at[h, c, d], ufar.at[c], agrecv.at[h + 1, c, d], 2 * toward[d] + core)
            if h == 0:
                if first_set:
                    continue
                for copy in ffn_loads:
                    copy.wait()
                arrived(wg.at[theirs], wrecv.at[0])
                arrived(wu.at[theirs], wrecv.at[1])
                arrived(wd.at[theirs], wrecv.at[2])
                expert_pair(ulr.at[h, 0, 0], ulr.at[h, 1, 1], part.at[h, 0])
            if first_set:
                expert_pair(ulr.at[h, 0, 0], ulr.at[h, 1, 1], part.at[h, 0])
            else:
                expert_pair(ulr.at[h, 1, 0], ulr.at[h, 0, 1], part.at[h, 1])
            if h == half - 2 and first_set:
                for d, g in both_ways:
                    pass_on(d, 1 - d, half - 1, g)
    for c in range(2):
        arrived(ufar.at[c], agrecv.at[half - 1, c, c])
    expert_pair(ufar.at[0], ufar.at[1], pfar)
    for d, g in both_ways:
        pass_on(d, d, half, g)

    arrived(uown, orecv.at[0])
    expert_pair(usend.at[core], uown, pown)
    remote(pown.at[pl.ds(seq, seq)], ownr, orecv.at[1], sibling)

    for r in range(half - 1):
        if half - 2 - r >= 1:
            for d, g in both_ways:
                add_and_pass(d, 1 - d, half - 2 - r, g)
        for d, g in both_ways:
            add_and_pass(d, d, half - 1 - r, g)

    arrived(ownr, orecv.at[1])
    for b in range(2):
        for d in range(2):
            for g in range(PIECES):
                arrived(fin.at[b, d, pl.ds(g * size, size)], finrecv.at[b, d, g])
    for b, own in ((core, pown.at[pl.ds(0, seq)]), (other, ownr)):
        hrow = pl.ds(pl.multiple_of(b * seq, seq), seq)
        out_ref[b] = (h_ref[hrow, :].astype(F32) + (own[...] + (fin[b, 0] + fin[b, 1]))).astype(BF16)
    local_copy(0, out_ref, out).wait()
    for copy in sends:
        copy.wait_send()


def solution(mesh):
    group = mesh.shape["ep"]
    row_spec = P(("dp", "ep"), None)
    full_spec = P(None, None, None)
    gain_spec = P(None)
    expert_spec = P("ep", None, None)
    in_specs = (row_spec,) * 8 + (gain_spec, full_spec, full_spec, full_spec, full_spec, gain_spec, expert_spec, expert_spec, expert_spec)

    def device_fn(tokens_a, experts_a, slots_a, gates_a, tokens_b, experts_b, slots_b, gates_b, attn_gain, w_query, w_key, w_value, w_out, moe_gain, w_gate, w_up, w_down):
        seq, dim = tokens_a.shape
        top_k = experts_a.shape[1]
        heads, head_dim = w_query.shape[1:]
        local, _, ffn = w_gate.shape
        half = group // 4
        both = 2 * seq
        urows = dim // LANES * seq
        urows_all = urows + local * group // 2

        def project(w):
            return w.transpose(1, 2, 0).reshape(heads * head_dim, dim)

        args = (
            tokens_a, experts_a.T, slots_a.T, gates_a.T, tokens_b, experts_b.T, slots_b.T, gates_b.T,
            attn_gain.reshape(dim // LANES, LANES), project(w_query), project(w_key), project(w_value),
            w_out.reshape(heads * head_dim, dim), moe_gain.reshape(dim // LANES, LANES), w_gate, w_up, w_down,
        )
        vmem = pltpu.VMEM
        scratch = [
            vmem((both, dim), BF16),
            vmem((2, top_k, seq), jnp.int32),
            vmem((2, top_k, seq), jnp.int32),
            vmem((2, top_k, seq), BF16),
            vmem((dim // LANES, LANES), BF16),
            vmem((dim // LANES, LANES), BF16),
            vmem((heads * head_dim, dim), BF16),
            vmem((heads * head_dim, dim), BF16),
            vmem((heads * head_dim, dim), BF16),
            vmem((heads * head_dim, dim), BF16),
            vmem((2 * local, dim, ffn), BF16),
            vmem((2 * local, dim, ffn), BF16),
            vmem((2 * local, ffn, dim), BF16),
            vmem((both, dim), BF16),
            vmem((both, dim), BF16),
            vmem((both, dim), BF16),
            vmem((both, dim), BF16),
            vmem((both, dim), BF16),
            vmem((both, dim), BF16),
            vmem((2, urows_all, LANES), BF16),
            vmem((urows_all, LANES), BF16),
            vmem((half - 1, 2, 2, urows_all, LANES), BF16),
            vmem((2, urows_all, LANES), BF16),
            vmem((local * group // 2, 2 * local * LANES), BF16),
            vmem((2 * local, both, LANES), F32),
            vmem((2 * local, both, ffn), BF16),
            vmem((half - 1, 2, both, dim), F32),
            vmem((both, dim), F32),
            vmem((both, dim), F32),
            vmem((2, half - 1, 2, seq, dim), F32),
            vmem((2, 2, seq, dim), F32),
            vmem((seq, dim), F32),
            vmem((2, seq, dim), BF16),
            pltpu.SemaphoreType.DMA((21,)),
            pltpu.SemaphoreType.DMA((9 + 4 * (half - 2) + 2 + 1 + (2 * half - 1) * 2 * PIECES,)),
            pltpu.SemaphoreType.DMA((3,)),
            pltpu.SemaphoreType.DMA((2,)),
            pltpu.SemaphoreType.DMA((half, 2, 2)),
            pltpu.SemaphoreType.DMA((2, half - 1, 2, PIECES)),
            pltpu.SemaphoreType.DMA((2, 2, PIECES)),
        ]
        rows_all = group * seq
        out = pl.pallas_call(
            functools.partial(layer_kernel, group),
            name="layer",
            out_shape=jax.ShapeDtypeStruct((2, seq, dim), BF16),
            in_specs=[pl.BlockSpec(memory_space=pl.ANY)] * len(args),
            out_specs=pl.BlockSpec(memory_space=pl.ANY),
            scratch_shapes=scratch,
            compiler_params=pltpu.CompilerParams(collective_id=0, has_side_effects=True, vmem_limit_bytes=60 * 1024 * 1024),
            cost_estimate=pl.CostEstimate(
                flops=rows_all * 6 * 2 * local * dim * ffn + both * 8 * dim * dim, bytes_accessed=2 * dim * (4 * dim + 3 * local * ffn), transcendentals=0
            ),
        )(*args)
        return out[0], out[1]

    return jax.shard_map(device_fn, mesh=mesh, in_specs=in_specs, out_specs=(row_spec, row_spec), check_vma=False)
```

```python
import functools

import jax
import jax.numpy as jnp
from jax import lax
from jax.experimental import pallas as pl
from jax.experimental.pallas import tpu as pltpu
from jax.sharding import PartitionSpec as P

NORM_EPS = 1e-6
MASK_VALUE = -1e30
LANES = 128
PIECES = 2
MESH = pl.DeviceIdType.MESH
NT = (((1,), (1,)), ((), ()))
TN = (((0,), (0,)), ((), ()))
F32 = jnp.float32
BF16 = jnp.bfloat16


def layer_kernel(
    group,
    tok_a, exp_a, slot_a, gate_a, tok_b, exp_b, slot_b, gate_b, attn_gain, wq_h, wk_h, wv_h, wo_h, moe_gain, wg_h, wu_h, wd_h,
    out,
    x_ref, exp_ref, slot_ref, gate_ref, again_ref, mgain_ref, wq, wk, wv, wo, wg, wu, wd,
    a_ref, q_ref, k_ref, v_ref, c_ref, h_ref, htmp, xsend, utmp, usend, uown, ulr, ufar, sel_ref, wbuf, hid_ref,
    part, pfar, pown, rbuf, fin, ownr,
    lsem, ssem, wrecv, orecv, agrecv, rsrecv, finrecv,
):
    seq, dim = tok_a.shape
    both = 2 * seq
    blocks = dim // LANES
    urows = blocks * seq
    local = wg_h.shape[0]
    experts = 2 * local
    ffn = wg_h.shape[2]
    top_k = exp_a.shape[0]
    chips = group // 2
    half = chips // 2
    gw_rows = local * group // 2

    me = lax.axis_index("ep")
    z = lax.div(me, 2)
    core = lax.rem(me, 2)
    other = 1 - core
    sibling = 2 * z + other
    right = lax.rem(z + 1, chips)
    left = lax.rem(z + chips - 1, chips)
    toward = (right, left)

    barrier = pltpu.get_barrier_semaphore()
    for peer in (2 * left, 2 * left + 1, 2 * right, 2 * right + 1, sibling):
        pl.semaphore_signal(barrier, inc=1, device_id={"ep": peer}, device_id_type=MESH)

    sends = []

    def local_copy(i, src, dst):
        copy = pltpu.make_async_copy(src, dst, lsem.at[i])
        copy.start()
        return copy

    def remote(src, dst, rsem, peer):
        copy = pltpu.make_async_remote_copy(
            src_ref=src, dst_ref=dst, send_sem=ssem.at[len(sends)], recv_sem=rsem, device_id={"ep": peer}, device_id_type=MESH
        )
        copy.start()
        sends.append(copy)

    def arrived(dst, rsem):
        pltpu.make_async_remote_copy(
            src_ref=dst, dst_ref=dst, send_sem=ssem.at[0], recv_sem=rsem, device_id={"ep": sibling}, device_id_type=MESH
        ).wait_recv()

    small = [local_copy(0, tok_a, x_ref.at[pl.ds(0, seq)]), local_copy(1, tok_b, x_ref.at[pl.ds(seq, seq)])]
    routes = [
        local_copy(7, exp_a, exp_ref.at[0]),
        local_copy(8, exp_b, exp_ref.at[1]),
        local_copy(9, slot_a, slot_ref.at[0]),
        local_copy(10, slot_b, slot_ref.at[1]),
        local_copy(11, gate_a, gate_ref.at[0]),
        local_copy(12, gate_b, gate_ref.at[1]),
        local_copy(2, attn_gain, again_ref),
        local_copy(3, moe_gain, mgain_ref),
    ]
    parts = [pl.ds(i * (dim // 4), dim // 4) for i in range(4)]
    loads = [[local_copy(17 + i, wq_h.at[rows], wq.at[rows]) for i, rows in enumerate(parts)]]
    loads += [[local_copy(5, wk_h, wk)], [local_copy(6, wv_h, wv)]]
    load_out = local_copy(13, wo_h, wo)
    mine = pl.ds(0, local)
    theirs = pl.ds(local, local)
    ffn_loads = [local_copy(14, wg_h, wg.at[mine]), local_copy(15, wu_h, wu.at[mine]), local_copy(16, wd_h, wd.at[mine])]

    pl.semaphore_wait(barrier, 5)
    remote(wg_h, wg.at[theirs], wrecv.at[0], sibling)
    remote(wu_h, wu.at[theirs], wrecv.at[1], sibling)
    remote(wd_h, wd.at[theirs], wrecv.at[2], sibling)

    for copy in small:
        copy.wait()
    for b in range(2):
        for j in range(blocks):
            xsend[b, j * seq:(j + 1) * seq, :] = x_ref[b * seq:(b + 1) * seq, j * LANES:(j + 1) * LANES]
    for copy in routes:
        copy.wait()
    eid = lax.broadcasted_iota(jnp.int32, (gw_rows, LANES), 0)
    eid = jnp.where(lax.broadcasted_iota(jnp.int32, (gw_rows, LANES), 1) >= seq, eid + gw_rows, eid)
    for b in range(2):
        ids = jnp.where(slot_ref[b] >= 0, exp_ref[b], -1)
        ids = jnp.concatenate([ids, ids], axis=1)
        gts = gate_ref[b].astype(F32)
        gts = jnp.concatenate([gts, gts], axis=1)
        gw = jnp.zeros((gw_rows, LANES), F32)
        for j in range(top_k):
            gw = gw + jnp.where(ids[j:j + 1, :] == eid, gts[j:j + 1, :], 0.0)
        xsend[b, pl.ds(urows, gw_rows), :] = gw.astype(BF16)
        usend[b, pl.ds(urows, gw_rows), :] = gw.astype(BF16)

    ways = (jnp.where(core == 0, right, left), jnp.where(core == 0, left, right))

    def first_hop(src, b, d, way):
        remote(src.at[b], ulr.at[0, core, d], agrecv.at[0, core, d], 2 * ways[way] + b)

    first_hop(xsend, core, core, 0)
    first_hop(xsend, other, core, 0)

    wide = 256
    row = lax.broadcasted_iota(jnp.int32, (2 * both, both), 0)
    col = lax.broadcasted_iota(jnp.int32, (2 * both, both), 1)
    row = jnp.where(row >= both, row - both, row)
    allowed = (row >= col) & ((row >= seq) == (col >= seq))
    low = lax.broadcasted_iota(jnp.int32, (both, LANES), 1) < LANES // 2
    scale = (LANES // 2) ** -0.5

    def scaled(xs, gain, j, inv):
        return (xs[:, j * LANES:(j + 1) * LANES] * inv * gain[j:j + 1, :]).astype(BF16)

    def attention(xs0, xs1, hdst, us0, us1, load=None, after_heads=None):
        gain = again_ref[...].astype(F32)
        for i in range(both // 16):
            sub, r = (xs0, i * 16) if i * 16 < seq else (xs1, i * 16 - seq)
            xs = jnp.concatenate([sub[pl.ds(j * seq + r, 16), :] for j in range(blocks)], axis=1).astype(F32)
            inv = lax.rsqrt(jnp.mean(xs * xs, axis=-1, keepdims=True) + NORM_EPS)
            for j in range(blocks):
                a_ref[i * 16:(i + 1) * 16, j * LANES:(j + 1) * LANES] = scaled(xs, gain, j, inv)
        for m, (w, dst) in enumerate(zip((wq, wk, wv), (q_ref, k_ref, v_ref))):
            for n in range(dim // LANES):
                if load is not None and n % (dim // LANES // len(load[m])) == 0:
                    load[m][n // (dim // LANES // len(load[m]))].wait()
                cols = slice(n * LANES, (n + 1) * LANES)
                dst[:, cols] = lax.dot_general(a_ref[...], w[cols, :], NT, preferred_element_type=F32).astype(BF16)
        for p in range(dim // LANES):
            cols = slice(p * LANES, (p + 1) * LANES)
            qp = q_ref[:, cols].astype(F32)
            vp = v_ref[:, cols].astype(F32)
            qq = jnp.concatenate([jnp.where(low, qp, 0.0), jnp.where(low, 0.0, qp)], axis=0).astype(BF16)
            vv = jnp.concatenate([jnp.where(low, vp, 0.0), jnp.where(low, 0.0, vp)], axis=0).astype(BF16)
            s = lax.dot_general(qq, k_ref[:, cols], NT, preferred_element_type=F32) * scale
            s = jnp.where(allowed, s, MASK_VALUE)
            e = jnp.exp(s - jnp.max(s, axis=-1, keepdims=True))
            prob = (e / jnp.sum(e, axis=-1, keepdims=True)).astype(BF16)
            pp = jnp.concatenate([prob[:both], prob[both:]], axis=1)
            c_ref[:, cols] = jnp.dot(pp, vv, preferred_element_type=F32).astype(BF16)
        if after_heads is not None:
            after_heads()
        if load is not None:
            load_out.wait()
        for n in range(dim // wide):
            cols = slice(n * wide, (n + 1) * wide)
            res = jnp.dot(c_ref[...], wo[:, cols], preferred_element_type=F32)
            per = wide // LANES
            xcols = jnp.concatenate(
                [jnp.concatenate([sub[pl.ds((n * per + m) * seq, seq), :] for m in range(per)], axis=1) for sub in (xs0, xs1)], axis=0
            )
            hdst[:, cols] = (xcols.astype(F32) + res).astype(BF16)
        gain = mgain_ref[...].astype(F32)
        for i in range(both // 16):
            sub, r = (us0, i * 16) if i * 16 < seq else (us1, i * 16 - seq)
            xs = hdst[i * 16:(i + 1) * 16, :].astype(F32)
            inv = lax.rsqrt(jnp.mean(xs * xs, axis=-1, keepdims=True) + NORM_EPS)
            for j in range(blocks):
                sub[pl.ds(j * seq + r, 16), :] = scaled(xs, gain, j, inv)

    def forward(h, c, d, peer):
        arrived(ulr.at[h, c, d], agrecv.at[h, c, d])
        if h + 1 < half - 1:
            remote(ulr.at[h, c, d], ulr.at[h + 1, c, d], agrecv.at[h + 1, c, d], 2 * peer + core)

    def forward_x(h):
        for d in range(2):
            forward(h, d, d, toward[d])
            if h + 1 == half - 1:
                remote(ulr.at[h, d, d], ufar.at[d], agrecv.at[h + 1, d, d], 2 * toward[d] + core)

    def forward_u(h):
        for d in range(2):
            forward(h, 1 - d, d, toward[d])

    attention(
        xsend.at[0], xsend.at[1], h_ref, usend.at[0], usend.at[1], loads, lambda: forward(0, core, core, ways[0])
    )
    forward(0, other, other, ways[1])
    remote(usend.at[other], uown, orecv.at[0], sibling)
    first_hop(usend, 0, other, 1)
    first_hop(usend, 1, other, 1)

    first = lax.rem(experts * z, gw_rows)
    upper = (experts * z) // gw_rows
    sel_row = lax.broadcasted_iota(jnp.int32, (gw_rows, experts * LANES), 0)
    sel_slot = lax.div(lax.broadcasted_iota(jnp.int32, (gw_rows, experts * LANES), 1), LANES)
    wanted = first + lax.rem(local * core + sel_slot, experts)
    sel_ref[...] = jnp.where(sel_row == wanted, 1.0, 0.0).astype(BF16)

    def gates_of(sub):
        packed = sub[pl.ds(urows, gw_rows), :]
        w = lax.dot_general(packed, sel_ref[...], TN, preferred_element_type=F32)
        return jnp.where(upper == 1, w[seq:], w[:seq])

    def expert_pair(us0, us1, sub0, sub1, dst):
        for i, sub in enumerate((sub0, sub1)):
            w = gates_of(sub)
            for k in range(experts):
                wbuf[k, i * seq:(i + 1) * seq, :] = w[:, k * LANES:(k + 1) * LANES]
        rows = jnp.concatenate(
            [jnp.concatenate([sub[j * seq:(j + 1) * seq, :] for j in range(blocks)], axis=1) for sub in (us0, us1)], axis=0
        )
        for k in range(experts):
            for n in range(ffn // wide):
                cols = slice(n * wide, (n + 1) * wide)
                g = jnp.dot(rows, wg[k, :, cols], preferred_element_type=F32)
                up = jnp.dot(rows, wu[k, :, cols], preferred_element_type=F32)
                hid_ref[k, :, cols] = (jax.nn.silu(g) * up).astype(BF16)
        for n in range(dim // wide):
            total = None
            for k in range(experts):
                o = jnp.dot(hid_ref[k], wd[k, :, n * wide:(n + 1) * wide], preferred_element_type=F32)
                o = o.astype(BF16).astype(F32)
                w = wbuf[k]
                term = jnp.concatenate(
                    [jnp.where(w > 0.0, w * o[:, m * LANES:(m + 1) * LANES], 0.0) for m in range(wide // LANES)], axis=1
                )
                total = term if total is None else total + term
            dst[:, n * wide:(n + 1) * wide] = total

    size = seq // PIECES

    def partial_of(d, c, k, g):
        if k == half:
            return pfar.at[pl.ds(c * seq + g * size, size)]
        came = 1 - d
        return part.at[k - 1, 0 if c == came else 1, pl.ds(came * seq + g * size, size)]

    def pass_on(d, c, k, g):
        src = partial_of(d, c, k, g)
        if k > 1:
            dst = rbuf.at[d, k - 2, c, pl.ds(g * size, size)]
            remote(src, dst, rsrecv.at[d, k - 2, c, g], 2 * toward[d] + core)
        else:
            dst = fin.at[core, d, pl.ds(g * size, size)]
            remote(src, dst, finrecv.at[core, d, g], 2 * toward[d] + c)

    def add_and_pass(d, c, k, g):
        got = rbuf.at[d, k - 1, c, pl.ds(g * size, size)]
        arrived(got, rsrecv.at[d, k - 1, c, g])
        mine_k = partial_of(d, c, k, g)
        mine_k[...] += got[...]
        pass_on(d, c, k, g)

    both_ways = [(d, g) for g in range(PIECES) for d in range(2)]

    def attention_x(h, after_heads=None):
        attention(ulr.at[h, 0, 0], ulr.at[h, 1, 1], htmp, utmp.at[h, 0], utmp.at[h, 1], None, after_heads)

    def experts_x(h):
        expert_pair(utmp.at[h, 0], utmp.at[h, 1], ulr.at[h, 0, 0], ulr.at[h, 1, 1], part.at[h, 0])

    def experts_u(h):
        subs = (ulr.at[h, 1, 0], ulr.at[h, 0, 1])
        expert_pair(*subs, *subs, part.at[h, 1])

    last = half - 2
    for h in range(last):
        if h > 0:
            forward_x(h)
        attention_x(h, functools.partial(forward_u, h - 1) if h > 0 else None)
        if h == last - 1:
            for copy in ffn_loads:
                copy.wait()
            arrived(wg.at[theirs], wrecv.at[0])
            arrived(wu.at[theirs], wrecv.at[1])
            arrived(wd.at[theirs], wrecv.at[2])
            experts_x(0)
    forward_x(last)
    attention_x(last, functools.partial(forward_u, last - 1))
    experts_x(last)
    for d, g in both_ways:
        pass_on(d, 1 - d, half - 1, g)
    for c in range(2):
        arrived(ufar.at[c], agrecv.at[half - 1, c, c])
    attention(ufar.at[0], ufar.at[1], htmp, utmp.at[half - 1, 0], utmp.at[half - 1, 1])
    expert_pair(utmp.at[half - 1, 0], utmp.at[half - 1, 1], ufar.at[0], ufar.at[1], pfar)
    for d, g in both_ways:
        pass_on(d, d, half, g)
    for h in range(1, last):
        experts_x(h)
    for d, g in both_ways:
        add_and_pass(d, 1 - d, half - 2, g)
    forward_u(last)
    experts_u(last)
    for d, g in both_ways:
        add_and_pass(d, d, half - 1, g)
    for h in range(last):
        experts_u(last - 1 - h)
    arrived(uown, orecv.at[0])
    expert_pair(usend.at[core], uown, usend.at[core], uown, pown)
    remote(pown.at[pl.ds(seq, seq)], ownr, orecv.at[1], sibling)

    for r in range(1, half - 1):
        if half - 2 - r >= 1:
            for d, g in both_ways:
                add_and_pass(d, 1 - d, half - 2 - r, g)
        for d, g in both_ways:
            add_and_pass(d, d, half - 1 - r, g)

    arrived(ownr, orecv.at[1])
    for g in range(PIECES):
        rows = pl.ds(g * size, size)
        for b in range(2):
            for d in range(2):
                arrived(fin.at[b, d, rows], finrecv.at[b, d, g])
        for b, own in ((core, pown.at[rows]), (other, ownr.at[rows])):
            hrow = pl.ds(pl.multiple_of(b * seq + g * size, size), size)
            out[b, rows, :] = (h_ref[hrow, :].astype(F32) + (own[...] + (fin[b, 0, rows, :] + fin[b, 1, rows, :]))).astype(BF16)
    for copy in sends:
        copy.wait_send()


def solution(mesh):
    group = mesh.shape["ep"]
    row_spec = P(("dp", "ep"), None)
    full_spec = P(None, None, None)
    gain_spec = P(None)
    expert_spec = P("ep", None, None)
    in_specs = (row_spec,) * 8 + (gain_spec, full_spec, full_spec, full_spec, full_spec, gain_spec, expert_spec, expert_spec, expert_spec)

    def device_fn(tokens_a, experts_a, slots_a, gates_a, tokens_b, experts_b, slots_b, gates_b, attn_gain, w_query, w_key, w_value, w_out, moe_gain, w_gate, w_up, w_down):
        seq, dim = tokens_a.shape
        top_k = experts_a.shape[1]
        heads, head_dim = w_query.shape[1:]
        local, _, ffn = w_gate.shape
        half = group // 4
        both = 2 * seq
        urows = dim // LANES * seq
        urows_all = urows + local * group // 2

        def project(w):
            return w.transpose(1, 2, 0).reshape(heads * head_dim, dim)

        args = (
            tokens_a, experts_a.T, slots_a.T, gates_a.T, tokens_b, experts_b.T, slots_b.T, gates_b.T,
            attn_gain.reshape(dim // LANES, LANES), project(w_query), project(w_key), project(w_value),
            w_out.reshape(heads * head_dim, dim), moe_gain.reshape(dim // LANES, LANES), w_gate, w_up, w_down,
        )
        vmem = pltpu.VMEM
        scratch = [
            vmem((both, dim), BF16),
            vmem((2, top_k, seq), jnp.int32),
            vmem((2, top_k, seq), jnp.int32),
            vmem((2, top_k, seq), BF16),
            vmem((dim // LANES, LANES), BF16),
            vmem((dim // LANES, LANES), BF16),
            vmem((heads * head_dim, dim), BF16),
            vmem((heads * head_dim, dim), BF16),
            vmem((heads * head_dim, dim), BF16),
            vmem((heads * head_dim, dim), BF16),
            vmem((2 * local, dim, ffn), BF16),
            vmem((2 * local, dim, ffn), BF16),
            vmem((2 * local, ffn, dim), BF16),
            vmem((both, dim), BF16),
            vmem((both, dim), BF16),
            vmem((both, dim), BF16),
            vmem((both, dim), BF16),
            vmem((both, dim), BF16),
            vmem((both, dim), BF16),
            vmem((both, dim), BF16),
            vmem((2, urows_all, LANES), BF16),
            vmem((half, 2, urows, LANES), BF16),
            vmem((2, urows_all, LANES), BF16),
            vmem((urows_all, LANES), BF16),
            vmem((half - 1, 2, 2, urows_all, LANES), BF16),
            vmem((2, urows_all, LANES), BF16),
            vmem((local * group // 2, 2 * local * LANES), BF16),
            vmem((2 * local, both, LANES), F32),
            vmem((2 * local, both, ffn), BF16),
            vmem((half - 1, 2, both, dim), F32),
            vmem((both, dim), F32),
            vmem((both, dim), F32),
            vmem((2, half - 1, 2, seq, dim), F32),
            vmem((2, 2, seq, dim), F32),
            vmem((seq, dim), F32),
            pltpu.SemaphoreType.DMA((21,)),
            pltpu.SemaphoreType.DMA((9 + 4 * (half - 2) + 2 + 1 + (2 * half - 1) * 2 * PIECES,)),
            pltpu.SemaphoreType.DMA((3,)),
            pltpu.SemaphoreType.DMA((2,)),
            pltpu.SemaphoreType.DMA((half, 2, 2)),
            pltpu.SemaphoreType.DMA((2, half - 1, 2, PIECES)),
            pltpu.SemaphoreType.DMA((2, 2, PIECES)),
        ]
        rows_all = group * seq
        out = pl.pallas_call(
            functools.partial(layer_kernel, group),
            name="layer",
            out_shape=pltpu.VMEM((2, seq, dim), BF16),
            in_specs=[pl.BlockSpec(memory_space=pl.ANY)] * len(args),
            out_specs=pl.BlockSpec(memory_space=pltpu.VMEM),
            scratch_shapes=scratch,
            compiler_params=pltpu.CompilerParams(collective_id=0, has_side_effects=True, vmem_limit_bytes=60 * 1024 * 1024),
            cost_estimate=pl.CostEstimate(
                flops=rows_all * 6 * 2 * local * dim * ffn + both * 8 * dim * dim, bytes_accessed=2 * dim * (4 * dim + 3 * local * ffn), transcendentals=0
            ),
        )(*args)
        return out[0], out[1]

    return jax.shard_map(device_fn, mesh=mesh, in_specs=in_specs, out_specs=(row_spec, row_spec), check_vma=False)
```

```python
import functools

import jax
import jax.numpy as jnp
from jax import lax
from jax.experimental import pallas as pl
from jax.experimental.pallas import tpu as pltpu
from jax.sharding import PartitionSpec as P

NORM_EPS = 1e-6
MASK_VALUE = -1e30
LANES = 128
PIECES = 2
MESH = pl.DeviceIdType.MESH
NT = (((1,), (1,)), ((), ()))
TN = (((0,), (0,)), ((), ()))
F32 = jnp.float32
BF16 = jnp.bfloat16


def layer_kernel(
    group,
    tok_a, exp_a, slot_a, gate_a, tok_b, exp_b, slot_b, gate_b, attn_gain, wq_h, wk_h, wv_h, wo_h, moe_gain, wg_h, wu_h, wd_h,
    out,
    x_ref, exp_ref, slot_ref, gate_ref, again_ref, mgain_ref, wq, wk, wv, wo, wg, wu, wd,
    a_ref, q_ref, k_ref, v_ref, c_ref, h_ref, htmp, xsend, utmp, usend, uown, ulr, ufar, sel_ref, wbuf, hid_ref,
    part, pfar, pown, rbuf, fin, ownr,
    lsem, ssem, wrecv, orecv, agrecv, rsrecv, finrecv,
):
    seq, dim = tok_a.shape
    both = 2 * seq
    blocks = dim // LANES
    urows = blocks * seq
    local = wg_h.shape[0]
    experts = 2 * local
    ffn = wg_h.shape[2]
    top_k = exp_a.shape[0]
    chips = group // 2
    half = chips // 2
    gw_rows = local * group // 2

    me = lax.axis_index("ep")
    z = lax.div(me, 2)
    core = lax.rem(me, 2)
    other = 1 - core
    sibling = 2 * z + other
    right = lax.rem(z + 1, chips)
    left = lax.rem(z + chips - 1, chips)
    toward = (right, left)

    barrier = pltpu.get_barrier_semaphore()
    for peer in (2 * left, 2 * left + 1, 2 * right, 2 * right + 1, sibling):
        pl.semaphore_signal(barrier, inc=1, device_id={"ep": peer}, device_id_type=MESH)

    sends = []

    def local_copy(i, src, dst):
        copy = pltpu.make_async_copy(src, dst, lsem.at[i])
        copy.start()
        return copy

    def remote(src, dst, rsem, peer):
        copy = pltpu.make_async_remote_copy(
            src_ref=src, dst_ref=dst, send_sem=ssem.at[len(sends)], recv_sem=rsem, device_id={"ep": peer}, device_id_type=MESH
        )
        copy.start()
        sends.append(copy)

    def arrived(dst, rsem):
        pltpu.make_async_remote_copy(
            src_ref=dst, dst_ref=dst, send_sem=ssem.at[0], recv_sem=rsem, device_id={"ep": sibling}, device_id_type=MESH
        ).wait_recv()

    small = [local_copy(0, tok_a, x_ref.at[pl.ds(0, seq)]), local_copy(1, tok_b, x_ref.at[pl.ds(seq, seq)])]
    routes = [
        local_copy(7, exp_a, exp_ref.at[0]),
        local_copy(8, exp_b, exp_ref.at[1]),
        local_copy(9, slot_a, slot_ref.at[0]),
        local_copy(10, slot_b, slot_ref.at[1]),
        local_copy(11, gate_a, gate_ref.at[0]),
        local_copy(12, gate_b, gate_ref.at[1]),
        local_copy(2, attn_gain, again_ref),
        local_copy(3, moe_gain, mgain_ref),
    ]
    parts = [pl.ds(i * (dim // 4), dim // 4) for i in range(4)]
    loads = [[local_copy(17 + i, wq_h.at[rows], wq.at[rows]) for i, rows in enumerate(parts)]]
    loads += [[local_copy(5, wk_h, wk)], [local_copy(6, wv_h, wv)]]
    load_out = local_copy(13, wo_h, wo)
    mine = pl.ds(0, local)
    theirs = pl.ds(local, local)
    ffn_loads = [local_copy(14, wg_h, wg.at[mine]), local_copy(15, wu_h, wu.at[mine]), local_copy(16, wd_h, wd.at[mine])]

    pl.semaphore_wait(barrier, 5)

    for copy in small:
        copy.wait()
    for b in range(2):
        for j in range(blocks):
            xsend[b, j * seq:(j + 1) * seq, :] = x_ref[b * seq:(b + 1) * seq, j * LANES:(j + 1) * LANES]
    for copy in routes:
        copy.wait()
    eid = lax.broadcasted_iota(jnp.int32, (gw_rows, LANES), 0)
    eid = jnp.where(lax.broadcasted_iota(jnp.int32, (gw_rows, LANES), 1) >= seq, eid + gw_rows, eid)
    for b in range(2):
        ids = jnp.where(slot_ref[b] >= 0, exp_ref[b], -1)
        ids = jnp.concatenate([ids, ids], axis=1)
        gts = gate_ref[b].astype(F32)
        gts = jnp.concatenate([gts, gts], axis=1)
        gw = jnp.zeros((gw_rows, LANES), F32)
        for j in range(top_k):
            gw = gw + jnp.where(ids[j:j + 1, :] == eid, gts[j:j + 1, :], 0.0)
        xsend[b, pl.ds(urows, gw_rows), :] = gw.astype(BF16)
        usend[b, pl.ds(urows, gw_rows), :] = gw.astype(BF16)

    ways = (jnp.where(core == 0, right, left), jnp.where(core == 0, left, right))

    def first_hop(src, b, d, way):
        remote(src.at[b], ulr.at[0, core, d], agrecv.at[0, core, d], 2 * ways[way] + b)

    first_hop(xsend, core, core, 0)
    first_hop(xsend, other, core, 0)
    remote(wg_h, wg.at[theirs], wrecv.at[0], sibling)
    remote(wu_h, wu.at[theirs], wrecv.at[1], sibling)
    remote(wd_h, wd.at[theirs], wrecv.at[2], sibling)

    wide = 256
    row = lax.broadcasted_iota(jnp.int32, (2 * both, both), 0)
    col = lax.broadcasted_iota(jnp.int32, (2 * both, both), 1)
    row = jnp.where(row >= both, row - both, row)
    allowed = (row >= col) & ((row >= seq) == (col >= seq))
    low = lax.broadcasted_iota(jnp.int32, (both, LANES), 1) < LANES // 2
    scale = (LANES // 2) ** -0.5

    def scaled(xs, gain, j, inv):
        return (xs[:, j * LANES:(j + 1) * LANES] * inv * gain[j:j + 1, :]).astype(BF16)

    def attention(xs0, xs1, hdst, us0, us1, load=None, after_heads=None):
        gain = again_ref[...].astype(F32)
        for i in range(both // 16):
            sub, r = (xs0, i * 16) if i * 16 < seq else (xs1, i * 16 - seq)
            xs = jnp.concatenate([sub[pl.ds(j * seq + r, 16), :] for j in range(blocks)], axis=1).astype(F32)
            inv = lax.rsqrt(jnp.mean(xs * xs, axis=-1, keepdims=True) + NORM_EPS)
            for j in range(blocks):
                a_ref[i * 16:(i + 1) * 16, j * LANES:(j + 1) * LANES] = scaled(xs, gain, j, inv)
        for m, (w, dst) in enumerate(zip((wq, wk, wv), (q_ref, k_ref, v_ref))):
            for n in range(dim // LANES):
                if load is not None and n % (dim // LANES // len(load[m])) == 0:
                    load[m][n // (dim // LANES // len(load[m]))].wait()
                cols = slice(n * LANES, (n + 1) * LANES)
                dst[:, cols] = lax.dot_general(a_ref[...], w[cols, :], NT, preferred_element_type=F32).astype(BF16)
        for p in range(dim // LANES):
            cols = slice(p * LANES, (p + 1) * LANES)
            qp = q_ref[:, cols].astype(F32)
            vp = v_ref[:, cols].astype(F32)
            qq = jnp.concatenate([jnp.where(low, qp, 0.0), jnp.where(low, 0.0, qp)], axis=0).astype(BF16)
            vv = jnp.concatenate([jnp.where(low, vp, 0.0), jnp.where(low, 0.0, vp)], axis=0).astype(BF16)
            s = lax.dot_general(qq, k_ref[:, cols], NT, preferred_element_type=F32) * scale
            s = jnp.where(allowed, s, MASK_VALUE)
            e = jnp.exp(s - jnp.max(s, axis=-1, keepdims=True))
            prob = (e / jnp.sum(e, axis=-1, keepdims=True)).astype(BF16)
            pp = jnp.concatenate([prob[:both], prob[both:]], axis=1)
            c_ref[:, cols] = jnp.dot(pp, vv, preferred_element_type=F32).astype(BF16)
        if after_heads is not None:
            after_heads()
        if load is not None:
            load_out.wait()
        for n in range(dim // wide):
            cols = slice(n * wide, (n + 1) * wide)
            res = jnp.dot(c_ref[...], wo[:, cols], preferred_element_type=F32)
            per = wide // LANES
            xcols = jnp.concatenate(
                [jnp.concatenate([sub[pl.ds((n * per + m) * seq, seq), :] for m in range(per)], axis=1) for sub in (xs0, xs1)], axis=0
            )
            hdst[:, cols] = (xcols.astype(F32) + res).astype(BF16)
        gain = mgain_ref[...].astype(F32)
        for i in range(both // 16):
            sub, r = (us0, i * 16) if i * 16 < seq else (us1, i * 16 - seq)
            xs = hdst[i * 16:(i + 1) * 16, :].astype(F32)
            inv = lax.rsqrt(jnp.mean(xs * xs, axis=-1, keepdims=True) + NORM_EPS)
            for j in range(blocks):
                sub[pl.ds(j * seq + r, 16), :] = scaled(xs, gain, j, inv)

    def forward(h, c, d, peer):
        arrived(ulr.at[h, c, d], agrecv.at[h, c, d])
        if h + 1 < half - 1:
            remote(ulr.at[h, c, d], ulr.at[h + 1, c, d], agrecv.at[h + 1, c, d], 2 * peer + core)

    def forward_x(h):
        for d in range(2):
            forward(h, d, d, toward[d])
            if h + 1 == half - 1:
                remote(ulr.at[h, d, d], ufar.at[d], agrecv.at[h + 1, d, d], 2 * toward[d] + core)

    def forward_u(h):
        for d in range(2):
            forward(h, 1 - d, d, toward[d])

    attention(
        xsend.at[0], xsend.at[1], h_ref, usend.at[0], usend.at[1], loads, lambda: forward(0, core, core, ways[0])
    )
    forward(0, other, other, ways[1])
    remote(usend.at[other], uown, orecv.at[0], sibling)
    first_hop(usend, 0, other, 1)
    first_hop(usend, 1, other, 1)

    first = lax.rem(experts * z, gw_rows)
    upper = (experts * z) // gw_rows
    sel_row = lax.broadcasted_iota(jnp.int32, (gw_rows, experts * LANES), 0)
    sel_slot = lax.div(lax.broadcasted_iota(jnp.int32, (gw_rows, experts * LANES), 1), LANES)
    wanted = first + lax.rem(local * core + sel_slot, experts)
    sel_ref[...] = jnp.where(sel_row == wanted, 1.0, 0.0).astype(BF16)

    def gates_of(sub):
        packed = sub[pl.ds(urows, gw_rows), :]
        w = lax.dot_general(packed, sel_ref[...], TN, preferred_element_type=F32)
        return jnp.where(upper == 1, w[seq:], w[:seq])

    def expert_pair(us0, us1, sub0, sub1, dst):
        for i, sub in enumerate((sub0, sub1)):
            w = gates_of(sub)
            for k in range(experts):
                wbuf[k, i * seq:(i + 1) * seq, :] = w[:, k * LANES:(k + 1) * LANES]
        rows = jnp.concatenate(
            [jnp.concatenate([sub[j * seq:(j + 1) * seq, :] for j in range(blocks)], axis=1) for sub in (us0, us1)], axis=0
        )
        for k in range(experts):
            for n in range(ffn // wide):
                cols = slice(n * wide, (n + 1) * wide)
                g = jnp.dot(rows, wg[k, :, cols], preferred_element_type=F32)
                up = jnp.dot(rows, wu[k, :, cols], preferred_element_type=F32)
                hid_ref[k, :, cols] = (jax.nn.silu(g) * up).astype(BF16)
        for n in range(dim // wide):
            total = None
            for k in range(experts):
                o = jnp.dot(hid_ref[k], wd[k, :, n * wide:(n + 1) * wide], preferred_element_type=F32)
                o = o.astype(BF16).astype(F32)
                w = wbuf[k]
                term = jnp.concatenate(
                    [jnp.where(w > 0.0, w * o[:, m * LANES:(m + 1) * LANES], 0.0) for m in range(wide // LANES)], axis=1
                )
                total = term if total is None else total + term
            dst[:, n * wide:(n + 1) * wide] = total

    size = seq // PIECES

    def partial_of(d, c, k, g):
        if k == half:
            return pfar.at[pl.ds(c * seq + g * size, size)]
        came = 1 - d
        return part.at[k - 1, 0 if c == came else 1, pl.ds(came * seq + g * size, size)]

    def pass_on(d, c, k, g):
        src = partial_of(d, c, k, g)
        if k > 1:
            dst = rbuf.at[d, k - 2, c, pl.ds(g * size, size)]
            remote(src, dst, rsrecv.at[d, k - 2, c, g], 2 * toward[d] + core)
        else:
            dst = fin.at[core, d, pl.ds(g * size, size)]
            remote(src, dst, finrecv.at[core, d, g], 2 * toward[d] + c)

    def add_and_pass(d, c, k, g):
        got = rbuf.at[d, k - 1, c, pl.ds(g * size, size)]
        arrived(got, rsrecv.at[d, k - 1, c, g])
        mine_k = partial_of(d, c, k, g)
        mine_k[...] += got[...]
        pass_on(d, c, k, g)

    both_ways = [(d, g) for g in range(PIECES) for d in range(2)]

    def attention_x(h, after_heads=None):
        attention(ulr.at[h, 0, 0], ulr.at[h, 1, 1], htmp, utmp.at[h, 0], utmp.at[h, 1], None, after_heads)

    def experts_x(h):
        expert_pair(utmp.at[h, 0], utmp.at[h, 1], ulr.at[h, 0, 0], ulr.at[h, 1, 1], part.at[h, 0])

    def experts_u(h):
        subs = (ulr.at[h, 1, 0], ulr.at[h, 0, 1])
        expert_pair(*subs, *subs, part.at[h, 1])

    last = half - 2
    for h in range(last):
        if h > 0:
            forward_x(h)
        attention_x(h, functools.partial(forward_u, h - 1) if h > 0 else None)
        if h == last - 1:
            for copy in ffn_loads:
                copy.wait()
            arrived(wg.at[theirs], wrecv.at[0])
            arrived(wu.at[theirs], wrecv.at[1])
            arrived(wd.at[theirs], wrecv.at[2])
            experts_x(0)
    forward_x(last)
    attention_x(last, functools.partial(forward_u, last - 1))
    experts_x(last)
    for d, g in both_ways:
        pass_on(d, 1 - d, half - 1, g)
    for c in range(2):
        arrived(ufar.at[c], agrecv.at[half - 1, c, c])
    attention(ufar.at[0], ufar.at[1], htmp, utmp.at[half - 1, 0], utmp.at[half - 1, 1])
    expert_pair(utmp.at[half - 1, 0], utmp.at[half - 1, 1], ufar.at[0], ufar.at[1], pfar)
    for d, g in both_ways:
        pass_on(d, d, half, g)
    for h in range(1, last):
        experts_x(h)
    for d, g in both_ways:
        add_and_pass(d, 1 - d, half - 2, g)
    forward_u(last)
    experts_u(last)
    for d, g in both_ways:
        add_and_pass(d, d, half - 1, g)
    for h in range(last):
        experts_u(last - 1 - h)
    arrived(uown, orecv.at[0])
    expert_pair(usend.at[core], uown, usend.at[core], uown, pown)
    remote(pown.at[pl.ds(seq, seq)], ownr, orecv.at[1], sibling)

    for r in range(1, half - 1):
        if half - 2 - r >= 1:
            for d, g in both_ways:
                add_and_pass(d, 1 - d, half - 2 - r, g)
        for d, g in both_ways:
            add_and_pass(d, d, half - 1 - r, g)

    arrived(ownr, orecv.at[1])
    for g in range(PIECES):
        rows = pl.ds(g * size, size)
        for b in range(2):
            for d in range(2):
                arrived(fin.at[b, d, rows], finrecv.at[b, d, g])
        for b, own in ((core, pown.at[rows]), (other, ownr.at[rows])):
            hrow = pl.ds(pl.multiple_of(b * seq + g * size, size), size)
            out[b, rows, :] = (h_ref[hrow, :].astype(F32) + (own[...] + (fin[b, 0, rows, :] + fin[b, 1, rows, :]))).astype(BF16)
    for copy in sends:
        copy.wait_send()


def solution(mesh):
    group = mesh.shape["ep"]
    row_spec = P(("dp", "ep"), None)
    full_spec = P(None, None, None)
    gain_spec = P(None)
    expert_spec = P("ep", None, None)
    in_specs = (row_spec,) * 8 + (gain_spec, full_spec, full_spec, full_spec, full_spec, gain_spec, expert_spec, expert_spec, expert_spec)

    def device_fn(tokens_a, experts_a, slots_a, gates_a, tokens_b, experts_b, slots_b, gates_b, attn_gain, w_query, w_key, w_value, w_out, moe_gain, w_gate, w_up, w_down):
        seq, dim = tokens_a.shape
        top_k = experts_a.shape[1]
        heads, head_dim = w_query.shape[1:]
        local, _, ffn = w_gate.shape
        half = group // 4
        both = 2 * seq
        urows = dim // LANES * seq
        urows_all = urows + local * group // 2

        def project(w):
            return w.transpose(1, 2, 0).reshape(heads * head_dim, dim)

        args = (
            tokens_a, experts_a.T, slots_a.T, gates_a.T, tokens_b, experts_b.T, slots_b.T, gates_b.T,
            attn_gain.reshape(dim // LANES, LANES), project(w_query), project(w_key), project(w_value),
            w_out.reshape(heads * head_dim, dim), moe_gain.reshape(dim // LANES, LANES), w_gate, w_up, w_down,
        )
        vmem = pltpu.VMEM
        scratch = [
            vmem((both, dim), BF16),
            vmem((2, top_k, seq), jnp.int32),
            vmem((2, top_k, seq), jnp.int32),
            vmem((2, top_k, seq), BF16),
            vmem((dim // LANES, LANES), BF16),
            vmem((dim // LANES, LANES), BF16),
            vmem((heads * head_dim, dim), BF16),
            vmem((heads * head_dim, dim), BF16),
            vmem((heads * head_dim, dim), BF16),
            vmem((heads * head_dim, dim), BF16),
            vmem((2 * local, dim, ffn), BF16),
            vmem((2 * local, dim, ffn), BF16),
            vmem((2 * local, ffn, dim), BF16),
            vmem((both, dim), BF16),
            vmem((both, dim), BF16),
            vmem((both, dim), BF16),
            vmem((both, dim), BF16),
            vmem((both, dim), BF16),
            vmem((both, dim), BF16),
            vmem((both, dim), BF16),
            vmem((2, urows_all, LANES), BF16),
            vmem((half, 2, urows, LANES), BF16),
            vmem((2, urows_all, LANES), BF16),
            vmem((urows_all, LANES), BF16),
            vmem((half - 1, 2, 2, urows_all, LANES), BF16),
            vmem((2, urows_all, LANES), BF16),
            vmem((local * group // 2, 2 * local * LANES), BF16),
            vmem((2 * local, both, LANES), F32),
            vmem((2 * local, both, ffn), BF16),
            vmem((half - 1, 2, both, dim), F32),
            vmem((both, dim), F32),
            vmem((both, dim), F32),
            vmem((2, half - 1, 2, seq, dim), F32),
            vmem((2, 2, seq, dim), F32),
            vmem((seq, dim), F32),
            pltpu.SemaphoreType.DMA((21,)),
            pltpu.SemaphoreType.DMA((9 + 4 * (half - 2) + 2 + 1 + (2 * half - 1) * 2 * PIECES,)),
            pltpu.SemaphoreType.DMA((3,)),
            pltpu.SemaphoreType.DMA((2,)),
            pltpu.SemaphoreType.DMA((half, 2, 2)),
            pltpu.SemaphoreType.DMA((2, half - 1, 2, PIECES)),
            pltpu.SemaphoreType.DMA((2, 2, PIECES)),
        ]
        rows_all = group * seq
        out = pl.pallas_call(
            functools.partial(layer_kernel, group),
            name="layer",
            out_shape=pltpu.VMEM((2, seq, dim), BF16),
            in_specs=[pl.BlockSpec(memory_space=pl.ANY)] * len(args),
            out_specs=pl.BlockSpec(memory_space=pltpu.VMEM),
            scratch_shapes=scratch,
            compiler_params=pltpu.CompilerParams(collective_id=0, has_side_effects=True, vmem_limit_bytes=60 * 1024 * 1024),
            cost_estimate=pl.CostEstimate(
                flops=rows_all * 6 * 2 * local * dim * ffn + both * 8 * dim * dim, bytes_accessed=2 * dim * (4 * dim + 3 * local * ffn), transcendentals=0
            ),
        )(*args)
        return out[0], out[1]

    return jax.shard_map(device_fn, mesh=mesh, in_specs=in_specs, out_specs=(row_spec, row_spec), check_vma=False)
```
